32 devices in a mesh: ba: 4 (over x, core), ma: 4 (over z), row: 2 (over y).
Axes of the slice: x: 2, y: 2, z: 4, core: 2. Of those that a mesh axis runs over, the one named last changes fastest.
Arguments:
- tokens: bfloat16 [8, 256, 4096], P(('ba', 'row'), None, 'ma'), may hold values from -6 to 6
- attn_gain: bfloat16 [4096], P('ma'), may hold values from 0.25 to 1.75
- query_weight: bfloat16 [4096, 4096], P('row', 'ma'), may hold values from -0.046875 to 0.046875
- key_weight: bfloat16 [4096, 4096], P('row', 'ma'), may hold values from -0.046875 to 0.046875
- value_projection_matrix: bfloat16 [4096, 4096], P('row', 'ma'), may hold values from -0.09375 to 0.09375
- attention_output_matrix: bfloat16 [4096, 4096], P('ma', 'row'), may hold values from -0.125 to 0.125
- bucket_bias_matrix: float32 [32, 64], P(None, 'ma'), may hold values from -6 to 215, as said below
- ffn_gain: bfloat16 [4096], P('ma'), may hold values from 0.25 to 1.75
- gate_weight: bfloat16 [4096, 8192], P(None, ('ma', 'row')), may hold values from -0.09375 to 0.09375
- up_weight: bfloat16 [4096, 8192], P(None, ('ma', 'row')), may hold values from -0.09375 to 0.09375
- down_projection_weight: bfloat16 [8192, 4096], P(('ma', 'row')), may hold values from -0.09375 to 0.09375
Outputs:
- encoded: bfloat16 [8, 256, 4096], P(('ba', 'row'), None, 'ma')
The draws below stay inside these ranges and needn't reach their ends.
Inputs may be any that keep to these rules, and one draw needn't show every extreme that they name: `bucket_bias_matrix`: entries of the relative position table.
All inputs are finite; a program needn't handle non-finite values.
Results may differ from the reference program's by a relative error of at most 0.017.
Values may be sent and summed in bfloat16 or wider, within the bound.
A program may use at most 128 MiB of HBM per device.

```python
import jax
import jax.numpy as jnp
from jax import lax

D = 4096
H = 64
DH = 64
FF = 8192
BUCKETS = 32
LEN = 256
BATCH = 8
N_MA = 4


def draw_bucket_bias_matrix(key, part):
    first_key, second_key = jax.random.split(key)
    normal_part = jnp.clip(jax.random.normal(first_key, (BUCKETS, H), jnp.float32), -6.0, 6.0)
    return normal_part


def spiked(entries, own_key, source, target, shards_of, factor):
    owner, partner = [(jnp.arange(entries.shape[axis_at]) // (entries.shape[axis_at] // shards_of)).reshape([-1 if axis == axis_at else 1 for axis in range(entries.ndim)]) for axis_at in (source, target)]
    chosen = jax.random.permutation(own_key, shards_of)[partner]
    strong = (owner == chosen) | (owner == (partner + shards_of // 2) % shards_of)
    return jnp.where(strong, factor * entries, entries)


def steps_of(stream_key, shape, cuts, smallest, largest):
    def one(position, shards_of):
        heights = jax.random.uniform(jax.random.fold_in(jax.random.fold_in(stream_key, 6), position), (shards_of,), jnp.float32, smallest / len(cuts), largest / len(cuts))
        return jnp.repeat(jnp.exp(heights), shape[position] // shards_of).reshape((-1,) + (1,) * (len(shape) - position - 1))

    loudness = one(*cuts[0])
    for cut in cuts[1:]:
        loudness = loudness * one(*cut)
    return loudness


def noise(stream_key, extent, spread, limit, cuts=(), held_as=jnp.bfloat16):
    loudness = steps_of(stream_key, extent, cuts, -0.22, 0.18) if cuts else 1.0
    entries = jax.random.normal(stream_key, extent, jnp.float32) * spread * loudness
    return jnp.minimum(jnp.maximum(entries, -limit), limit).astype(held_as)


def noise_with(rng, dims, deviation, most, pieces, heavy, kind=jnp.bfloat16):
    result = deviation * jax.random.normal(rng, dims, jnp.float32)
    if pieces:
        result = result * steps_of(rng, dims, pieces, -0.22, 0.18)
    return jnp.clip(spiked(result, jax.random.fold_in(rng, 3), *heavy), -most, most).astype(kind)


def setup_inputs(seed: int = 0) -> dict:
    key_of = jax.random.split(jax.random.key(seed), 12)
    tokens = noise(key_of[0], (BATCH, LEN, D), 1.0, 6.0, ((0, 8), (2, 4)))
    attn_gain = jnp.clip(1.0 + 0.15 * jax.random.normal(key_of[1], (D,), jnp.float32), 0.25, 1.75).astype(jnp.bfloat16)
    query_weight = noise(key_of[2], (D, H * DH), (4 * D) ** -0.5, 0.046875, ((0, 2), (1, 4)))
    key_weight = noise(key_of[3], (D, H * DH), (4 * D) ** -0.5, 0.046875, ((0, 2), (1, 4)))
    value_projection_matrix = noise(key_of[4], (D, H * DH), D ** -0.5, 0.09375, ((0, 2), (1, 4)))
    attention_output_matrix = noise_with(key_of[5], (H * DH, D), (H * DH) ** -0.5, 0.125, ((0, 4), (1, 2)), (0, 1, 4, 2.0))
    bucket_bias_matrix = draw_bucket_bias_matrix(jax.random.fold_in(key_of[11], 71), 0)
    ffn_gain = jnp.clip(1.0 + 0.15 * jax.random.normal(key_of[7], (D,), jnp.float32), 0.25, 1.75).astype(jnp.bfloat16)
    gate_weight = noise(key_of[8], (D, FF), D ** -0.5, 0.09375, ((1, 8),))
    up_weight = noise(key_of[9], (D, FF), D ** -0.5, 0.09375, ((1, 8),))
    down_projection_weight = noise_with(key_of[10], (FF, D), FF ** -0.5, 0.09375, ((0, 8),), (0, 1, 8, 2.0))
    return dict(tokens=tokens, attn_gain=attn_gain, query_weight=query_weight, key_weight=key_weight, value_projection_matrix=value_projection_matrix, attention_output_matrix=attention_output_matrix, bucket_bias_matrix=bucket_bias_matrix, ffn_gain=ffn_gain, gate_weight=gate_weight, up_weight=up_weight, down_projection_weight=down_projection_weight)


bucket_thresholds = (1, 2, 3, 4, 5, 6, 7, 8, 11, 16, 23, 32, 45, 64, 91, 128)
epsilon = 1e-06

def buckets(length):
    places = jnp.arange(length, dtype=jnp.int32)
    offset = places[None, :] - places[:, None]
    distance = jnp.abs(offset)
    backward = jnp.zeros_like(distance)
    for threshold in bucket_thresholds[:15]:
        backward = backward + (distance >= threshold).astype(jnp.int32)
    forward = jnp.full_like(distance, 15)
    for threshold in bucket_thresholds:
        forward = forward + (distance >= threshold).astype(jnp.int32)
    return jnp.where(offset > 0, forward, backward)

def rms_scale(values, gain):
    mean_square = lax.optimization_barrier(jnp.mean(values * values, axis=-1, keepdims=True))
    return (values * lax.rsqrt(mean_square + epsilon) * gain.astype(jnp.float32)).astype(jnp.bfloat16)

def grouped_sum(left, right, groups):
    span = left.shape[1] // groups

    def add_group(running, group_index):
        columns = lax.dynamic_slice_in_dim(left, group_index * span, span, 1)
        matrix = lax.dynamic_slice_in_dim(right, group_index * span, span, 0)
        partial_term = jnp.dot(columns, matrix, preferred_element_type=jnp.float32).astype(jnp.bfloat16)
        partial_term = lax.optimization_barrier(partial_term).astype(jnp.float32)
        return (running + partial_term, None)
    start_sum = jnp.zeros((left.shape[0], right.shape[1]), jnp.float32)
    total, unused = lax.scan(add_group, start_sum, jnp.arange(groups, dtype=jnp.int32))
    return total

def reference(tokens, attn_gain, query_weight, key_weight, value_projection_matrix, attention_output_matrix, bucket_bias_matrix, ffn_gain, gate_weight, up_weight, down_projection_weight):
    batch_size, length, model_width = tokens.shape
    head_count = bucket_bias_matrix.shape[1]
    inner_width = query_weight.shape[1]
    head_size = inner_width // head_count
    token_rows = tokens.reshape(batch_size * length, model_width).astype(jnp.float32)
    normed = rms_scale(token_rows, attn_gain)
    projected = tuple((jnp.dot(normed, matrix, preferred_element_type=jnp.float32).astype(jnp.bfloat16).reshape(batch_size, length, head_count, head_size) for matrix in (query_weight, key_weight, value_projection_matrix)))
    relative_position_scores = jnp.transpose(bucket_bias_matrix[buckets(length)], (2, 0, 1))

    def attend(inputs):
        query_heads, key_heads, value_heads = inputs
        scores = jnp.einsum('qhd,khd->hqk', query_heads.astype(jnp.float32), key_heads.astype(jnp.float32)) + relative_position_scores
        row_max = lax.optimization_barrier(jnp.max(scores, axis=-1, keepdims=True))
        exponent = jnp.exp(scores - row_max)
        weights = (exponent / lax.optimization_barrier(jnp.sum(exponent, axis=-1, keepdims=True))).astype(jnp.bfloat16)
        return jnp.einsum('hqk,khd->qhd', weights.astype(jnp.float32), value_heads.astype(jnp.float32)).astype(jnp.bfloat16)
    attended = lax.map(attend, projected).reshape(batch_size * length, inner_width)
    attn_out = grouped_sum(attended, attention_output_matrix, N_MA)
    residual_stream = (token_rows + attn_out).astype(jnp.bfloat16)
    residual_f = residual_stream.astype(jnp.float32)
    ffn_in = rms_scale(residual_f, ffn_gain)
    gate_act = jnp.dot(ffn_in, gate_weight, preferred_element_type=jnp.float32)
    up_act = jnp.dot(ffn_in, up_weight, preferred_element_type=jnp.float32)
    hidden = (jax.nn.gelu(gate_act, approximate=True) * up_act).astype(jnp.bfloat16)
    ffn_out = jnp.dot(hidden, down_projection_weight, preferred_element_type=jnp.float32)
    encoded = (residual_f + ffn_out).astype(jnp.bfloat16)
    return encoded.reshape(batch_size, length, model_width)
```

```python
import jax
import jax.numpy as jnp
from jax import lax
from jax.sharding import PartitionSpec as P

bucket_thresholds = (1, 2, 3, 4, 5, 6, 7, 8, 11, 16, 23, 32, 45, 64, 91, 128)
epsilon = 1e-06


def buckets(length):
    places = jnp.arange(length, dtype=jnp.int32)
    offset = places[None, :] - places[:, None]
    distance = jnp.abs(offset)
    backward = jnp.zeros_like(distance)
    for threshold in bucket_thresholds[:15]:
        backward = backward + (distance >= threshold).astype(jnp.int32)
    forward = jnp.full_like(distance, 15)
    for threshold in bucket_thresholds:
        forward = forward + (distance >= threshold).astype(jnp.int32)
    return jnp.where(offset > 0, forward, backward)


def rms_scale(values, gain):
    mean_square = jnp.mean(values * values, axis=-1, keepdims=True)
    return (values * lax.rsqrt(mean_square + epsilon) * gain.astype(jnp.float32)).astype(
        jnp.bfloat16
    )


def on_device(
    tokens,
    attn_gain,
    query_weight,
    key_weight,
    value_projection_matrix,
    attention_output_matrix,
    bucket_bias_matrix,
    ffn_gain,
    gate_weight,
    up_weight,
    down_projection_weight,
):
    sequences, length, part_width = tokens.shape
    ma_count = lax.axis_size("ma")
    local_heads = bucket_bias_matrix.shape[1]
    inner_width = query_weight.shape[1]
    head_size = inner_width // local_heads
    slab_rows = sequences * length
    token_rows = tokens.reshape(slab_rows, part_width)
    token_float = token_rows.astype(jnp.float32)
    row_count = lax.axis_size("row")
    half = query_weight.shape[0]
    swap = [(i, i ^ 1) for i in range(row_count)]
    my_row = lax.axis_index("row")
    gains = jnp.concatenate(
        [attn_gain.reshape(1, part_width), ffn_gain.reshape(1, part_width)]
        + [jnp.zeros((14, part_width), jnp.bfloat16)]
    )
    whole = lax.all_gather(jnp.concatenate([token_rows, gains]), "ma", axis=1, tiled=True)
    whole_rows = whole[:slab_rows]
    ffn_gain_full = whole[slab_rows + 1]
    normed = rms_scale(whole_rows.astype(jnp.float32), whole[slab_rows])
    mine = lax.dynamic_slice_in_dim(normed, my_row * half, half, 1)
    theirs = lax.dynamic_slice_in_dim(normed, (1 - my_row) * half, half, 1)
    arrived = lax.ppermute(theirs, "row", swap)
    weights_qkv = (query_weight, key_weight, value_projection_matrix)
    outgoing = [
        jnp.dot(arrived, matrix, preferred_element_type=jnp.float32).astype(jnp.bfloat16)
        for matrix in weights_qkv
    ]
    incoming = [lax.ppermute(part, "row", swap) for part in outgoing]
    projected = [
        jnp.dot(mine, matrix, preferred_element_type=jnp.float32) + part.astype(jnp.float32)
        for matrix, part in zip(weights_qkv, incoming)
    ]
    query_heads, key_heads, value_heads = [
        member.astype(jnp.bfloat16).reshape(sequences, length, local_heads, head_size)
        for member in projected
    ]
    bucket_grid = buckets(length)
    table_rows = jnp.arange(bucket_bias_matrix.shape[0], dtype=jnp.int32)
    bucket_indicator = (table_rows[:, None, None] == bucket_grid[None, :, :]).astype(jnp.float32)
    relative_position_scores = jnp.einsum(
        "dmy,du->umy", bucket_indicator, bucket_bias_matrix, precision=lax.Precision.HIGHEST
    )
    scores = (
        jnp.einsum("sqhd,skhd->shqk", query_heads, key_heads, preferred_element_type=jnp.float32)
        + relative_position_scores[None]
    )
    row_max = jnp.max(scores, axis=-1, keepdims=True)
    exponent = jnp.exp(scores - row_max)
    weights = (exponent / jnp.sum(exponent, axis=-1, keepdims=True)).astype(jnp.bfloat16)
    attended = jnp.einsum(
        "shqk,skhd->sqhd", weights, value_heads, preferred_element_type=jnp.float32
    )
    attended = attended.astype(jnp.bfloat16).reshape(slab_rows, inner_width)
    attended_peer = lax.ppermute(attended, "row", swap)
    sent_out = jnp.dot(
        attended_peer, attention_output_matrix, preferred_element_type=jnp.float32
    ).astype(jnp.bfloat16)
    other_half = lax.ppermute(sent_out, "row", swap)
    own_half = jnp.dot(
        attended, attention_output_matrix, preferred_element_type=jnp.float32
    ).astype(jnp.bfloat16)
    partial_out = jnp.where(
        my_row == 0,
        jnp.concatenate([own_half, other_half], axis=1),
        jnp.concatenate([other_half, own_half], axis=1),
    )
    attn_out = lax.psum_scatter(
        partial_out.astype(jnp.bfloat16), "ma", scatter_dimension=1, tiled=True
    ).astype(jnp.float32)
    residual_stream = (token_float + attn_out).astype(jnp.bfloat16)
    residual_f = residual_stream.astype(jnp.float32)
    gate_full, up_full, down_full = (gate_weight, up_weight, down_projection_weight)
    group_rows = lax.all_gather(
        lax.all_gather(residual_stream, "ma", axis=1, tiled=True), "row", axis=0, tiled=True
    )
    ffn_in = rms_scale(group_rows.astype(jnp.float32), ffn_gain_full)
    gate_act = jnp.dot(ffn_in, gate_full, preferred_element_type=jnp.float32)
    up_act = jnp.dot(ffn_in, up_full, preferred_element_type=jnp.float32)
    hidden = (jax.nn.gelu(gate_act, approximate=True) * up_act).astype(jnp.bfloat16)
    down_blocks = down_full.reshape(down_full.shape[0], ma_count, part_width)
    down_terms = jnp.einsum("tf,fmd->mtd", hidden, down_blocks, preferred_element_type=jnp.float32)
    down_terms = down_terms.reshape(ma_count * ffn_in.shape[0], part_width)
    ffn_out = lax.psum_scatter(
        down_terms.astype(jnp.bfloat16), ("ma", "row"), scatter_dimension=0, tiled=True
    ).astype(jnp.float32)
    encoded = (residual_f + ffn_out).astype(jnp.bfloat16)
    return encoded.reshape(sequences, length, part_width)


def solution(mesh):
    in_specs = (
        P(("ba", "row"), None, "ma"),
        P("ma"),
        P("row", "ma"),
        P("row", "ma"),
        P("row", "ma"),
        P("ma", "row"),
        P(None, "ma"),
        P("ma"),
        P(None, ("ma", "row")),
        P(None, ("ma", "row")),
        P(("ma", "row"), None),
    )
    out_specs = P(("ba", "row"), None, "ma")
    return jax.shard_map(
        on_device, mesh=mesh, in_specs=in_specs, out_specs=out_specs, check_vma=False
    )
```

```python
import functools

import jax
import jax.numpy as jnp
from jax import lax
from jax.experimental import pallas as pl
from jax.experimental.pallas import tpu as pltpu
from jax.sharding import PartitionSpec as P

bucket_thresholds = (1, 2, 3, 4, 5, 6, 7, 8, 11, 16, 23, 32, 45, 64, 91, 128)
epsilon = 1e-06


def buckets(length):
    places = jnp.arange(length, dtype=jnp.int32)
    offset = places[None, :] - places[:, None]
    distance = jnp.abs(offset)
    backward = jnp.zeros_like(distance)
    for threshold in bucket_thresholds[:15]:
        backward = backward + (distance >= threshold).astype(jnp.int32)
    forward = jnp.full_like(distance, 15)
    for threshold in bucket_thresholds:
        forward = forward + (distance >= threshold).astype(jnp.int32)
    return jnp.where(offset > 0, forward, backward)


def rms_scale(values, gain):
    mean_square = jnp.mean(values * values, axis=-1, keepdims=True)
    return (values * lax.rsqrt(mean_square + epsilon) * gain.astype(jnp.float32)).astype(
        jnp.bfloat16
    )


MESH = pl.DeviceIdType.MESH


def greet(me, count, row):
    barrier = pltpu.get_barrier_semaphore()

    @pl.when(me > 0)
    def _():
        pl.semaphore_signal(barrier, inc=1, device_id={"ma": me - 1}, device_id_type=MESH)

    @pl.when(me < count - 1)
    def _():
        pl.semaphore_signal(barrier, inc=1, device_id={"ma": me + 1}, device_id_type=MESH)

    pl.semaphore_signal(barrier, inc=1, device_id={"row": 1 - row}, device_id_type=MESH)
    inner = jnp.logical_and(me > 0, me < count - 1)
    pl.semaphore_wait(barrier, jnp.where(inner, 3, 2))


def gather_kernel(count, pieces, x_ref, out_ref, local_sem, send_sem, z_sem, y_sem):
    me = lax.axis_index("ma")
    row = lax.axis_index("row")
    length, width = x_ref.shape
    step_rows = length // pieces
    greet(me, count, row)

    def place(block, piece, which):
        return out_ref.at[
            pl.ds(pl.multiple_of(which * length + piece * step_rows, step_rows), step_rows),
            pl.ds(pl.multiple_of(block * width, width), width),
        ]

    def copy(way, block, piece, src=None):
        here = place(block, piece, row)
        target = ({"ma": me + 1}, {"ma": me - 1}, {"row": 1 - row})[way]
        sem = y_sem if way == 2 else z_sem
        return pltpu.make_async_remote_copy(
            src_ref=here if src is None else src,
            dst_ref=here,
            send_sem=send_sem.at[way, block, piece],
            recv_sem=sem.at[block, piece],
            device_id=target,
            device_id_type=MESH,
        )

    def own(piece):
        return x_ref.at[pl.ds(piece * step_rows, step_rows), :]

    for piece in range(pieces):

        @pl.when(me < count - 1)
        def _():
            copy(0, me, piece, own(piece)).start()

        @pl.when(me > 0)
        def _():
            copy(1, me, piece, own(piece)).start()

        copy(2, me, piece, own(piece)).start()
    mine = pltpu.make_async_copy(
        x_ref,
        out_ref.at[
            pl.ds(pl.multiple_of(row * length, length), length),
            pl.ds(pl.multiple_of(me * width, width), width),
        ],
        local_sem,
    )
    mine.start()
    for step in range(1, count):
        for piece in range(pieces):

            @pl.when(me - step >= 0)
            def _():
                block = me - step
                copy(0, block, piece).wait_recv()

                @pl.when(me < count - 1)
                def _():
                    copy(0, block, piece).start()

                copy(2, block, piece).start()

            @pl.when(me + step < count)
            def _():
                block = me + step
                copy(1, block, piece).wait_recv()

                @pl.when(me > 0)
                def _():
                    copy(1, block, piece).start()

                copy(2, block, piece).start()

    mine.wait()
    for block in range(count):
        for piece in range(pieces):
            here = place(block, piece, 1 - row)
            pltpu.make_async_remote_copy(
                src_ref=here,
                dst_ref=here,
                send_sem=send_sem.at[2, block, piece],
                recv_sem=y_sem.at[block, piece],
                device_id={"row": 1 - row},
                device_id_type=MESH,
            ).wait_recv()
            copy(2, block, piece).wait_send()

            @pl.when(jnp.logical_and(me < count - 1, block <= me))
            def _():
                copy(0, block, piece).wait_send()

            @pl.when(jnp.logical_and(me > 0, block >= me))
            def _():
                copy(1, block, piece).wait_send()


def gather_all(values, count, pieces, collective_id):
    length, width = values.shape
    return pl.pallas_call(
        functools.partial(gather_kernel, count, pieces),
        out_shape=jax.ShapeDtypeStruct((2 * length, count * width), values.dtype),
        in_specs=[pl.BlockSpec(memory_space=pltpu.VMEM)],
        out_specs=pl.BlockSpec(memory_space=pltpu.VMEM),
        scratch_shapes=[
            pltpu.SemaphoreType.DMA,
            pltpu.SemaphoreType.DMA((3, count, pieces)),
            pltpu.SemaphoreType.DMA((count, pieces)),
            pltpu.SemaphoreType.DMA((count, pieces)),
        ],
        compiler_params=pltpu.CompilerParams(collective_id=collective_id, has_side_effects=True),
    )(values)


def reduce_kernel(
    count, hidden_ref, down_ref, out_ref, sent, landed, total, left_in, right_in,
    right_out, left_out, y_send, y_recv, r_send, r_recv, l_send, l_recv
):
    me = lax.axis_index("ma")
    row = lax.axis_index("row")
    length, width = out_ref.shape
    greet(me, count, row)

    def y_copy(block):
        return pltpu.make_async_remote_copy(
            src_ref=sent.at[block],
            dst_ref=landed.at[block],
            send_sem=y_send.at[block],
            recv_sem=y_recv.at[block],
            device_id={"row": 1 - row},
            device_id_type=MESH,
        )

    def r_copy(block):
        return pltpu.make_async_remote_copy(
            src_ref=right_out.at[block],
            dst_ref=left_in.at[block],
            send_sem=r_send.at[block],
            recv_sem=r_recv.at[block],
            device_id={"ma": me + 1},
            device_id_type=MESH,
        )

    def l_copy(block):
        return pltpu.make_async_remote_copy(
            src_ref=left_out.at[block],
            dst_ref=right_in.at[block],
            send_sem=l_send.at[block],
            recv_sem=l_recv.at[block],
            device_id={"ma": me - 1},
            device_id_type=MESH,
        )

    def product(which, block):
        rows = hidden_ref[pl.ds(pl.multiple_of(which * length, length), length), :]
        columns = pl.ds(pl.multiple_of(block * width, width), width)
        return jnp.dot(rows, down_ref[:, columns], preferred_element_type=jnp.float32)

    def ordered(body):
        def turn(index, carry):
            step = count - 1 - index // 2
            rightward = index % 2 == 0
            block = jnp.where(rightward, me + step, me - step)
            inside = jnp.logical_and(block >= 0, block < count)

            @pl.when(jnp.logical_and(inside, jnp.logical_or(step > 0, rightward)))
            def _():
                body(block)

            return carry

        lax.fori_loop(0, 2 * count, turn, 0)

    def send_peer(block):
        sent[block] = product(1 - row, block).astype(jnp.bfloat16)
        y_copy(block).start()

    ordered(send_peer)

    def pass_on(block):
        total[...] = product(row, block)
        y_copy(block).wait_recv()
        total[...] = total[...] + landed[block].astype(jnp.float32)

        @pl.when(jnp.logical_and(block >= me, me > 0))
        def _():
            r_copy(block).wait_recv()
            total[...] = total[...] + left_in[block].astype(jnp.float32)

        @pl.when(jnp.logical_and(block <= me, me < count - 1))
        def _():
            l_copy(block).wait_recv()
            total[...] = total[...] + right_in[block].astype(jnp.float32)

        @pl.when(block > me)
        def _():
            right_out[block] = total[...].astype(jnp.bfloat16)
            r_copy(block).start()

        @pl.when(block < me)
        def _():
            left_out[block] = total[...].astype(jnp.bfloat16)
            l_copy(block).start()

        @pl.when(block == me)
        def _():
            out_ref[...] = total[...]

    ordered(pass_on)
    for block in range(count):
        y_copy(block).wait_send()

        @pl.when(block > me)
        def _():
            r_copy(block).wait_send()

        @pl.when(block < me)
        def _():
            l_copy(block).wait_send()


def reduce_all(hidden, down, count, collective_id):
    length = hidden.shape[0] // 2
    width = down.shape[1] // count
    blocks = pltpu.VMEM((count, length, width), jnp.bfloat16)
    return pl.pallas_call(
        functools.partial(reduce_kernel, count),
        out_shape=jax.ShapeDtypeStruct((length, width), jnp.float32),
        in_specs=[pl.BlockSpec(memory_space=pltpu.VMEM)] * 2,
        out_specs=pl.BlockSpec(memory_space=pltpu.VMEM),
        scratch_shapes=[
            blocks,
            blocks,
            pltpu.VMEM((length, width), jnp.float32),
            blocks,
            blocks,
            blocks,
            blocks,
        ]
        + [pltpu.SemaphoreType.DMA((count,))] * 6,
        compiler_params=pltpu.CompilerParams(
            collective_id=collective_id, has_side_effects=True, vmem_limit_bytes=60 * 2**20
        ),
    )(hidden, down)


def on_device(
    tokens,
    attn_gain,
    query_weight,
    key_weight,
    value_projection_matrix,
    attention_output_matrix,
    bucket_bias_matrix,
    ffn_gain,
    gate_weight,
    up_weight,
    down_projection_weight,
):
    sequences, length, part_width = tokens.shape
    ma_count = lax.axis_size("ma")
    local_heads = bucket_bias_matrix.shape[1]
    inner_width = query_weight.shape[1]
    head_size = inner_width // local_heads
    slab_rows = sequences * length
    token_rows = tokens.reshape(slab_rows, part_width)
    token_float = token_rows.astype(jnp.float32)
    row_count = lax.axis_size("row")
    half = query_weight.shape[0]
    swap = [(i, i ^ 1) for i in range(row_count)]
    my_row = lax.axis_index("row")
    gains = jnp.concatenate(
        [attn_gain.reshape(1, part_width), ffn_gain.reshape(1, part_width)]
        + [jnp.zeros((14, part_width), jnp.bfloat16)]
    )
    whole = lax.all_gather(jnp.concatenate([token_rows, gains]), "ma", axis=1, tiled=True)
    whole_rows = whole[:slab_rows]
    ffn_gain_full = whole[slab_rows + 1]
    normed = rms_scale(whole_rows.astype(jnp.float32), whole[slab_rows])
    mine = lax.dynamic_slice_in_dim(normed, my_row * half, half, 1)
    theirs = lax.dynamic_slice_in_dim(normed, (1 - my_row) * half, half, 1)
    arrived = lax.ppermute(theirs, "row", swap)
    weights_qkv = (query_weight, key_weight, value_projection_matrix)
    outgoing = [
        jnp.dot(arrived, matrix, preferred_element_type=jnp.float32).astype(jnp.bfloat16)
        for matrix in weights_qkv
    ]
    incoming = [lax.ppermute(part, "row", swap) for part in outgoing]
    projected = [
        jnp.dot(mine, matrix, preferred_element_type=jnp.float32) + part.astype(jnp.float32)
        for matrix, part in zip(weights_qkv, incoming)
    ]
    query_heads, key_heads, value_heads = [
        member.astype(jnp.bfloat16).reshape(sequences, length, local_heads, head_size)
        for member in projected
    ]
    bucket_grid = buckets(length)
    table_rows = jnp.arange(bucket_bias_matrix.shape[0], dtype=jnp.int32)
    bucket_indicator = (table_rows[:, None, None] == bucket_grid[None, :, :]).astype(jnp.float32)
    relative_position_scores = jnp.einsum(
        "dmy,du->umy", bucket_indicator, bucket_bias_matrix, precision=lax.Precision.HIGHEST
    )
    scores = (
        jnp.einsum("sqhd,skhd->shqk", query_heads, key_heads, preferred_element_type=jnp.float32)
        + relative_position_scores[None]
    )
    row_max = jnp.max(scores, axis=-1, keepdims=True)
    exponent = jnp.exp(scores - row_max)
    weights = (exponent / jnp.sum(exponent, axis=-1, keepdims=True)).astype(jnp.bfloat16)
    attended = jnp.einsum(
        "shqk,skhd->sqhd", weights, value_heads, preferred_element_type=jnp.float32
    )
    attended = attended.astype(jnp.bfloat16).reshape(slab_rows, inner_width)
    attended_peer = lax.ppermute(attended, "row", swap)
    sent_out = jnp.dot(
        attended_peer, attention_output_matrix, preferred_element_type=jnp.float32
    ).astype(jnp.bfloat16)
    other_half = lax.ppermute(sent_out, "row", swap)
    own_half = jnp.dot(
        attended, attention_output_matrix, preferred_element_type=jnp.float32
    ).astype(jnp.bfloat16)
    partial_out = jnp.where(
        my_row == 0,
        jnp.concatenate([own_half, other_half], axis=1),
        jnp.concatenate([other_half, own_half], axis=1),
    )
    attn_out = lax.psum_scatter(
        partial_out.astype(jnp.bfloat16), "ma", scatter_dimension=1, tiled=True
    ).astype(jnp.float32)
    residual_stream = (token_float + attn_out).astype(jnp.bfloat16)
    residual_f = residual_stream.astype(jnp.float32)
    gate_full, up_full, down_full = (gate_weight, up_weight, down_projection_weight)
    group_rows = gather_all(residual_stream, ma_count, 2, 0)
    ffn_in = rms_scale(group_rows.astype(jnp.float32), ffn_gain_full)
    gate_act = jnp.dot(ffn_in, gate_full, preferred_element_type=jnp.float32)
    up_act = jnp.dot(ffn_in, up_full, preferred_element_type=jnp.float32)
    hidden = (jax.nn.gelu(gate_act, approximate=True) * up_act).astype(jnp.bfloat16)
    ffn_out = reduce_all(hidden, down_full, ma_count, 1)
    encoded = (residual_f + ffn_out).astype(jnp.bfloat16)
    return encoded.reshape(sequences, length, part_width)


def solution(mesh):
    in_specs = (
        P(("ba", "row"), None, "ma"),
        P("ma"),
        P("row", "ma"),
        P("row", "ma"),
        P("row", "ma"),
        P("ma", "row"),
        P(None, "ma"),
        P("ma"),
        P(None, ("ma", "row")),
        P(None, ("ma", "row")),
        P(("ma", "row"), None),
    )
    out_specs = P(("ba", "row"), None, "ma")
    return jax.shard_map(
        on_device, mesh=mesh, in_specs=in_specs, out_specs=out_specs, check_vma=False
    )
```

```python
import functools

import jax
import jax.numpy as jnp
from jax import lax
from jax.experimental import pallas as pl
from jax.experimental.pallas import tpu as pltpu
from jax.sharding import PartitionSpec as P

bucket_thresholds = (1, 2, 3, 4, 5, 6, 7, 8, 11, 16, 23, 32, 45, 64, 91, 128)
epsilon = 1e-06


def buckets(length):
    places = jnp.arange(length, dtype=jnp.int32)
    offset = places[None, :] - places[:, None]
    distance = jnp.abs(offset)
    backward = jnp.zeros_like(distance)
    for threshold in bucket_thresholds[:15]:
        backward = backward + (distance >= threshold).astype(jnp.int32)
    forward = jnp.full_like(distance, 15)
    for threshold in bucket_thresholds:
        forward = forward + (distance >= threshold).astype(jnp.int32)
    return jnp.where(offset > 0, forward, backward)


def rms_scale(values, gain):
    mean_square = jnp.mean(values * values, axis=-1, keepdims=True)
    return (values * lax.rsqrt(mean_square + epsilon) * gain.astype(jnp.float32)).astype(
        jnp.bfloat16
    )


MESH = pl.DeviceIdType.MESH


def greet(me, count, row):
    barrier = pltpu.get_barrier_semaphore()

    @pl.when(me > 0)
    def _():
        pl.semaphore_signal(barrier, inc=1, device_id={"ma": me - 1}, device_id_type=MESH)

    @pl.when(me < count - 1)
    def _():
        pl.semaphore_signal(barrier, inc=1, device_id={"ma": me + 1}, device_id_type=MESH)

    pl.semaphore_signal(barrier, inc=1, device_id={"row": 1 - row}, device_id_type=MESH)
    inner = jnp.logical_and(me > 0, me < count - 1)
    pl.semaphore_wait(barrier, jnp.where(inner, 3, 2))


def gather_kernel(count, pieces, x_ref, out_ref, local_sem, send_sem, z_sem, y_sem):
    me = lax.axis_index("ma")
    row = lax.axis_index("row")
    length, width = x_ref.shape
    step_rows = length // pieces
    greet(me, count, row)

    def place(block, piece, which):
        return out_ref.at[
            pl.ds(pl.multiple_of(which * length + piece * step_rows, step_rows), step_rows),
            pl.ds(pl.multiple_of(block * width, width), width),
        ]

    def copy(way, block, piece, src=None):
        here = place(block, piece, row)
        target = ({"ma": me + 1}, {"ma": me - 1}, {"row": 1 - row})[way]
        sem = y_sem if way == 2 else z_sem
        return pltpu.make_async_remote_copy(
            src_ref=here if src is None else src,
            dst_ref=here,
            send_sem=send_sem.at[way, block, piece],
            recv_sem=sem.at[block, piece],
            device_id=target,
            device_id_type=MESH,
        )

    def own(piece):
        return x_ref.at[pl.ds(piece * step_rows, step_rows), :]

    for piece in range(pieces):

        @pl.when(me < count - 1)
        def _():
            copy(0, me, piece, own(piece)).start()

        @pl.when(me > 0)
        def _():
            copy(1, me, piece, own(piece)).start()

        copy(2, me, piece, own(piece)).start()
    mine = pltpu.make_async_copy(
        x_ref,
        out_ref.at[
            pl.ds(pl.multiple_of(row * length, length), length),
            pl.ds(pl.multiple_of(me * width, width), width),
        ],
        local_sem,
    )
    mine.start()
    for step in range(1, count):
        for piece in range(pieces):

            @pl.when(me - step >= 0)
            def _():
                block = me - step
                copy(0, block, piece).wait_recv()

                @pl.when(me < count - 1)
                def _():
                    copy(0, block, piece).start()

                copy(2, block, piece).start()

            @pl.when(me + step < count)
            def _():
                block = me + step
                copy(1, block, piece).wait_recv()

                @pl.when(me > 0)
                def _():
                    copy(1, block, piece).start()

                copy(2, block, piece).start()

    mine.wait()
    for block in range(count):
        for piece in range(pieces):
            here = place(block, piece, 1 - row)
            pltpu.make_async_remote_copy(
                src_ref=here,
                dst_ref=here,
                send_sem=send_sem.at[2, block, piece],
                recv_sem=y_sem.at[block, piece],
                device_id={"row": 1 - row},
                device_id_type=MESH,
            ).wait_recv()
            copy(2, block, piece).wait_send()

            @pl.when(jnp.logical_and(me < count - 1, block <= me))
            def _():
                copy(0, block, piece).wait_send()

            @pl.when(jnp.logical_and(me > 0, block >= me))
            def _():
                copy(1, block, piece).wait_send()


def gather_all(values, count, pieces, collective_id):
    length, width = values.shape
    return pl.pallas_call(
        functools.partial(gather_kernel, count, pieces),
        out_shape=jax.ShapeDtypeStruct((2 * length, count * width), values.dtype),
        in_specs=[pl.BlockSpec(memory_space=pltpu.VMEM)],
        out_specs=pl.BlockSpec(memory_space=pltpu.VMEM),
        scratch_shapes=[
            pltpu.SemaphoreType.DMA,
            pltpu.SemaphoreType.DMA((3, count, pieces)),
            pltpu.SemaphoreType.DMA((count, pieces)),
            pltpu.SemaphoreType.DMA((count, pieces)),
        ],
        compiler_params=pltpu.CompilerParams(collective_id=collective_id, has_side_effects=True),
    )(values)


def reduce_kernel(count, pieces, paired, left_ref, right_ref, out_ref, *scratch):
    if paired:
        sent, landed, y_send, y_recv = scratch[:4]
    total, left_in, right_in, right_out, left_out, r_send, r_recv, l_send, l_recv = scratch[-9:]
    me = lax.axis_index("ma")
    row = lax.axis_index("row")
    length, width = out_ref.shape
    step_rows = length // pieces
    greet(me, count, row)

    def y_copy(unit):
        return pltpu.make_async_remote_copy(
            src_ref=sent.at[unit],
            dst_ref=landed.at[unit],
            send_sem=y_send.at[unit],
            recv_sem=y_recv.at[unit],
            device_id={"row": 1 - row},
            device_id_type=MESH,
        )

    def r_copy(unit):
        return pltpu.make_async_remote_copy(
            src_ref=right_out.at[unit],
            dst_ref=left_in.at[unit],
            send_sem=r_send.at[unit],
            recv_sem=r_recv.at[unit],
            device_id={"ma": me + 1},
            device_id_type=MESH,
        )

    def l_copy(unit):
        return pltpu.make_async_remote_copy(
            src_ref=left_out.at[unit],
            dst_ref=right_in.at[unit],
            send_sem=l_send.at[unit],
            recv_sem=l_recv.at[unit],
            device_id={"ma": me - 1},
            device_id_type=MESH,
        )

    def product(which, block, piece):
        start = pl.multiple_of(which * length + piece * step_rows, step_rows)
        columns = pl.ds(pl.multiple_of(block * width, width), width)
        return jnp.dot(
            left_ref[pl.ds(start, step_rows), :],
            right_ref[:, columns],
            preferred_element_type=jnp.float32,
        )

    def ordered(body):
        def turn(index, carry):
            piece = index % pieces
            side = index // pieces
            step = count - 1 - side // 2
            rightward = side % 2 == 0
            block = jnp.where(rightward, me + step, me - step)
            inside = jnp.logical_and(block >= 0, block < count)

            @pl.when(jnp.logical_and(inside, jnp.logical_or(step > 0, rightward)))
            def _():
                body(block, piece, block * pieces + piece)

            return carry

        lax.fori_loop(0, 2 * count * pieces, turn, 0)

    def send_peer(block, piece, unit):
        sent[unit] = product(1 - row, block, piece).astype(jnp.bfloat16)
        y_copy(unit).start()

    if paired:
        ordered(send_peer)

    def pass_on(block, piece, unit):
        total[...] = product(row if paired else 0, block, piece)
        if paired:
            y_copy(unit).wait_recv()
            total[...] = total[...] + landed[unit].astype(jnp.float32)

        @pl.when(jnp.logical_and(block >= me, me > 0))
        def _():
            r_copy(unit).wait_recv()
            total[...] = total[...] + left_in[unit].astype(jnp.float32)

        @pl.when(jnp.logical_and(block <= me, me < count - 1))
        def _():
            l_copy(unit).wait_recv()
            total[...] = total[...] + right_in[unit].astype(jnp.float32)

        @pl.when(block > me)
        def _():
            right_out[unit] = total[...].astype(jnp.bfloat16)
            r_copy(unit).start()

        @pl.when(block < me)
        def _():
            left_out[unit] = total[...].astype(jnp.bfloat16)
            l_copy(unit).start()

        @pl.when(block == me)
        def _():
            out_ref[pl.ds(pl.multiple_of(piece * step_rows, step_rows), step_rows), :] = total[...]

    ordered(pass_on)

    def drain(unit, carry):
        block = unit // pieces
        if paired:
            y_copy(unit).wait_send()

        @pl.when(block > me)
        def _():
            r_copy(unit).wait_send()

        @pl.when(block < me)
        def _():
            l_copy(unit).wait_send()

        return carry

    lax.fori_loop(0, count * pieces, drain, 0)


def reduce_all(left, right, count, pieces, paired, collective_id):
    length = left.shape[0] // (2 if paired else 1)
    width = right.shape[1] // count
    units = count * pieces
    blocks = pltpu.VMEM((units, length // pieces, width), jnp.bfloat16)
    sems = pltpu.SemaphoreType.DMA((units,))
    return pl.pallas_call(
        functools.partial(reduce_kernel, count, pieces, paired),
        out_shape=jax.ShapeDtypeStruct((length, width), jnp.float32),
        in_specs=[pl.BlockSpec(memory_space=pltpu.VMEM)] * 2,
        out_specs=pl.BlockSpec(memory_space=pltpu.VMEM),
        scratch_shapes=([blocks, blocks, sems, sems] if paired else [])
        + [pltpu.VMEM((length // pieces, width), jnp.float32)]
        + [blocks] * 4
        + [sems] * 4,
        compiler_params=pltpu.CompilerParams(
            collective_id=collective_id, has_side_effects=True, vmem_limit_bytes=60 * 2**20
        ),
    )(left, right)


def on_device(
    tokens,
    attn_gain,
    query_weight,
    key_weight,
    value_projection_matrix,
    attention_output_matrix,
    bucket_bias_matrix,
    ffn_gain,
    gate_weight,
    up_weight,
    down_projection_weight,
):
    sequences, length, part_width = tokens.shape
    ma_count = lax.axis_size("ma")
    local_heads = bucket_bias_matrix.shape[1]
    inner_width = query_weight.shape[1]
    head_size = inner_width // local_heads
    slab_rows = sequences * length
    token_rows = tokens.reshape(slab_rows, part_width)
    token_float = token_rows.astype(jnp.float32)
    row_count = lax.axis_size("row")
    half = query_weight.shape[0]
    swap = [(i, i ^ 1) for i in range(row_count)]
    my_row = lax.axis_index("row")
    ba_count = lax.axis_size("ba")
    lane = lax.axis_index("ba") % 2
    half_rows = attention_output_matrix.shape[0] // 2
    out_piece = lax.dynamic_slice_in_dim(attention_output_matrix, lane * half_rows, half_rows, 0)
    out_other = lax.ppermute(out_piece, "row", swap)
    out_rest = lax.ppermute(out_other, "ba", [(i, i ^ 1) for i in range(ba_count)])
    gains = jnp.concatenate(
        [attn_gain.reshape(1, part_width), ffn_gain.reshape(1, part_width)]
        + [jnp.zeros((14, part_width), jnp.bfloat16)]
    )
    whole = lax.all_gather(jnp.concatenate([token_rows, gains]), "ma", axis=1, tiled=True)
    whole_rows = whole[:slab_rows]
    ffn_gain_full = whole[slab_rows + 1]
    normed = rms_scale(whole_rows.astype(jnp.float32), whole[slab_rows])
    mine = lax.dynamic_slice_in_dim(normed, my_row * half, half, 1)
    theirs = lax.dynamic_slice_in_dim(normed, (1 - my_row) * half, half, 1)
    arrived = lax.ppermute(theirs, "row", swap)
    weights_qkv = (query_weight, key_weight, value_projection_matrix)
    outgoing = [
        jnp.dot(arrived, matrix, preferred_element_type=jnp.float32).astype(jnp.bfloat16)
        for matrix in weights_qkv
    ]
    incoming = [lax.ppermute(part, "row", swap) for part in outgoing]
    projected = [
        jnp.dot(mine, matrix, preferred_element_type=jnp.float32) + part.astype(jnp.float32)
        for matrix, part in zip(weights_qkv, incoming)
    ]
    query_heads, key_heads, value_heads = [
        member.astype(jnp.bfloat16).reshape(sequences, length, local_heads, head_size)
        for member in projected
    ]
    bucket_grid = buckets(length)
    table_rows = jnp.arange(bucket_bias_matrix.shape[0], dtype=jnp.int32)
    bucket_indicator = (table_rows[:, None, None] == bucket_grid[None, :, :]).astype(jnp.float32)
    relative_position_scores = jnp.einsum(
        "dmy,du->umy", bucket_indicator, bucket_bias_matrix, precision=lax.Precision.HIGHEST
    )
    scores = (
        jnp.einsum("sqhd,skhd->shqk", query_heads, key_heads, preferred_element_type=jnp.float32)
        + relative_position_scores[None]
    )
    row_max = jnp.max(scores, axis=-1, keepdims=True)
    exponent = jnp.exp(scores - row_max)
    weights = (exponent / jnp.sum(exponent, axis=-1, keepdims=True)).astype(jnp.bfloat16)
    attended = jnp.einsum(
        "shqk,skhd->sqhd", weights, value_heads, preferred_element_type=jnp.float32
    )
    attended = attended.astype(jnp.bfloat16).reshape(slab_rows, inner_width)
    out_far = jnp.where(
        lane == 0,
        jnp.concatenate([out_other, out_rest]),
        jnp.concatenate([out_rest, out_other]),
    )
    out_full = jnp.where(
        my_row == 0,
        jnp.concatenate([attention_output_matrix, out_far], axis=1),
        jnp.concatenate([out_far, attention_output_matrix], axis=1),
    )
    attn_out = reduce_all(attended, out_full, ma_count, 2, False, 2)
    residual_stream = (token_float + attn_out).astype(jnp.bfloat16)
    residual_f = residual_stream.astype(jnp.float32)
    gate_full, up_full, down_full = (gate_weight, up_weight, down_projection_weight)
    group_rows = gather_all(residual_stream, ma_count, 2, 0)
    ffn_in = rms_scale(group_rows.astype(jnp.float32), ffn_gain_full)
    gate_act = jnp.dot(ffn_in, gate_full, preferred_element_type=jnp.float32)
    up_act = jnp.dot(ffn_in, up_full, preferred_element_type=jnp.float32)
    hidden = (jax.nn.gelu(gate_act, approximate=True) * up_act).astype(jnp.bfloat16)
    ffn_out = reduce_all(hidden, down_full, ma_count, 2, True, 1)
    encoded = (residual_f + ffn_out).astype(jnp.bfloat16)
    return encoded.reshape(sequences, length, part_width)


def solution(mesh):
    in_specs = (
        P(("ba", "row"), None, "ma"),
        P("ma"),
        P("row", "ma"),
        P("row", "ma"),
        P("row", "ma"),
        P("ma", "row"),
        P(None, "ma"),
        P("ma"),
        P(None, ("ma", "row")),
        P(None, ("ma", "row")),
        P(("ma", "row"), None),
    )
    out_specs = P(("ba", "row"), None, "ma")
    return jax.shard_map(
        on_device, mesh=mesh, in_specs=in_specs, out_specs=out_specs, check_vma=False
    )
```

```python
import functools

import jax
import jax.numpy as jnp
from jax import lax
from jax.experimental import pallas as pl
from jax.experimental.pallas import tpu as pltpu
from jax.sharding import PartitionSpec as P

bucket_thresholds = (1, 2, 3, 4, 5, 6, 7, 8, 11, 16, 23, 32, 45, 64, 91, 128)
epsilon = 1e-06


def buckets(length):
    places = jnp.arange(length, dtype=jnp.int32)
    offset = places[None, :] - places[:, None]
    distance = jnp.abs(offset)
    backward = jnp.zeros_like(distance)
    for threshold in bucket_thresholds[:15]:
        backward = backward + (distance >= threshold).astype(jnp.int32)
    forward = jnp.full_like(distance, 15)
    for threshold in bucket_thresholds:
        forward = forward + (distance >= threshold).astype(jnp.int32)
    return jnp.where(offset > 0, forward, backward)


def rms_scale(values, gain):
    mean_square = jnp.mean(values * values, axis=-1, keepdims=True)
    return (values * lax.rsqrt(mean_square + epsilon) * gain.astype(jnp.float32)).astype(
        jnp.bfloat16
    )


MESH = pl.DeviceIdType.MESH


def greet(me, count, row):
    barrier = pltpu.get_barrier_semaphore()

    @pl.when(me > 0)
    def _():
        pl.semaphore_signal(barrier, inc=1, device_id={"ma": me - 1}, device_id_type=MESH)

    @pl.when(me < count - 1)
    def _():
        pl.semaphore_signal(barrier, inc=1, device_id={"ma": me + 1}, device_id_type=MESH)

    pl.semaphore_signal(barrier, inc=1, device_id={"row": 1 - row}, device_id_type=MESH)
    inner = jnp.logical_and(me > 0, me < count - 1)
    pl.semaphore_wait(barrier, jnp.where(inner, 3, 2))


def gather_kernel(count, cuts, halved, x_ref, out_ref, local_sem, send_sem, z_sem, y_sem):
    me = lax.axis_index("ma")
    row = lax.axis_index("row")
    length, width = x_ref.shape
    pieces = len(cuts) - 1
    greet(me, count, row)

    def leaves(block):
        return block // (count // 2) == 1 - row if halved else block >= 0

    def comes(block):
        return block // (count // 2) == row if halved else block >= 0

    def place(block, piece, which):
        return out_ref.at[
            pl.ds(pl.multiple_of(which * length + cuts[piece], 16), cuts[piece + 1] - cuts[piece]),
            pl.ds(pl.multiple_of(block * width, width), width),
        ]

    def copy(way, block, piece, src=None):
        here = place(block, piece, row)
        target = ({"ma": me + 1}, {"ma": me - 1}, {"row": 1 - row})[way]
        sem = y_sem if way == 2 else z_sem
        return pltpu.make_async_remote_copy(
            src_ref=here if src is None else src,
            dst_ref=here,
            send_sem=send_sem.at[way, block, piece],
            recv_sem=sem.at[block, piece],
            device_id=target,
            device_id_type=MESH,
        )

    def own(piece):
        return x_ref.at[pl.ds(cuts[piece], cuts[piece + 1] - cuts[piece]), :]

    for piece in range(pieces):

        @pl.when(me < count - 1)
        def _():
            copy(0, me, piece, own(piece)).start()

        @pl.when(me > 0)
        def _():
            copy(1, me, piece, own(piece)).start()

        @pl.when(leaves(me))
        def _():
            copy(2, me, piece, own(piece)).start()

    mine = pltpu.make_async_copy(
        x_ref,
        out_ref.at[
            pl.ds(pl.multiple_of(row * length, length), length),
            pl.ds(pl.multiple_of(me * width, width), width),
        ],
        local_sem,
    )
    mine.start()
    for step in range(1, count):
        for piece in range(pieces):

            @pl.when(me - step >= 0)
            def _():
                block = me - step
                copy(0, block, piece).wait_recv()

                @pl.when(me < count - 1)
                def _():
                    copy(0, block, piece).start()

                @pl.when(leaves(block))
                def _():
                    copy(2, block, piece).start()

            @pl.when(me + step < count)
            def _():
                block = me + step
                copy(1, block, piece).wait_recv()

                @pl.when(me > 0)
                def _():
                    copy(1, block, piece).start()

                @pl.when(leaves(block))
                def _():
                    copy(2, block, piece).start()

    mine.wait()
    for block in range(count):
        for piece in range(pieces):
            here = place(block, piece, 1 - row)
            arrival = pltpu.make_async_remote_copy(
                src_ref=here,
                dst_ref=here,
                send_sem=send_sem.at[2, block, piece],
                recv_sem=y_sem.at[block, piece],
                device_id={"row": 1 - row},
                device_id_type=MESH,
            )

            @pl.when(comes(jnp.int32(block)))
            def _():
                arrival.wait_recv()

            @pl.when(leaves(jnp.int32(block)))
            def _():
                copy(2, block, piece).wait_send()

            @pl.when(jnp.logical_and(me < count - 1, block <= me))
            def _():
                copy(0, block, piece).wait_send()

            @pl.when(jnp.logical_and(me > 0, block >= me))
            def _():
                copy(1, block, piece).wait_send()


def gather_all(values, count, cuts, halved, collective_id):
    length, width = values.shape
    pieces = len(cuts) - 1
    return pl.pallas_call(
        functools.partial(gather_kernel, count, cuts, halved),
        out_shape=jax.ShapeDtypeStruct((2 * length, count * width), values.dtype),
        in_specs=[pl.BlockSpec(memory_space=pltpu.VMEM)],
        out_specs=pl.BlockSpec(memory_space=pltpu.VMEM),
        scratch_shapes=[
            pltpu.SemaphoreType.DMA,
            pltpu.SemaphoreType.DMA((3, count, pieces)),
            pltpu.SemaphoreType.DMA((count, pieces)),
            pltpu.SemaphoreType.DMA((count, pieces)),
        ],
        compiler_params=pltpu.CompilerParams(collective_id=collective_id, has_side_effects=True),
    )(values)


def reduce_kernel(count, pieces, paired, left_ref, right_ref, out_ref, *scratch):
    if paired:
        sent, landed, y_send, y_recv = scratch[:4]
    total, left_in, right_in, right_out, left_out, r_send, r_recv, l_send, l_recv = scratch[-9:]
    me = lax.axis_index("ma")
    row = lax.axis_index("row")
    length, width = out_ref.shape
    step_rows = length // pieces
    greet(me, count, row)

    def y_copy(unit):
        return pltpu.make_async_remote_copy(
            src_ref=sent.at[unit],
            dst_ref=landed.at[unit],
            send_sem=y_send.at[unit],
            recv_sem=y_recv.at[unit],
            device_id={"row": 1 - row},
            device_id_type=MESH,
        )

    def r_copy(unit):
        return pltpu.make_async_remote_copy(
            src_ref=right_out.at[unit],
            dst_ref=left_in.at[unit],
            send_sem=r_send.at[unit],
            recv_sem=r_recv.at[unit],
            device_id={"ma": me + 1},
            device_id_type=MESH,
        )

    def l_copy(unit):
        return pltpu.make_async_remote_copy(
            src_ref=left_out.at[unit],
            dst_ref=right_in.at[unit],
            send_sem=l_send.at[unit],
            recv_sem=l_recv.at[unit],
            device_id={"ma": me - 1},
            device_id_type=MESH,
        )

    def product(which, block, piece):
        start = pl.multiple_of(which * length + piece * step_rows, step_rows)
        columns = pl.ds(pl.multiple_of(block * width, width), width)
        return jnp.dot(
            left_ref[pl.ds(start, step_rows), :],
            right_ref[:, columns],
            preferred_element_type=jnp.float32,
        )

    def ordered(body):
        def turn(index, carry):
            piece = index % pieces
            side = index // pieces
            step = count - 1 - side // 2
            rightward = side % 2 == 0
            block = jnp.where(rightward, me + step, me - step)
            inside = jnp.logical_and(block >= 0, block < count)

            @pl.when(jnp.logical_and(inside, jnp.logical_or(step > 0, rightward)))
            def _():
                body(block, piece, block * pieces + piece)

            return carry

        lax.fori_loop(0, 2 * count * pieces, turn, 0)

    def send_peer(block, piece, unit):
        sent[unit] = product(1 - row, block, piece).astype(jnp.bfloat16)
        y_copy(unit).start()

    if paired:
        ordered(send_peer)

    def pass_on(block, piece, unit):
        total[...] = product(row if paired else 0, block, piece)
        if paired:
            y_copy(unit).wait_recv()
            total[...] = total[...] + landed[unit].astype(jnp.float32)

        @pl.when(jnp.logical_and(block >= me, me > 0))
        def _():
            r_copy(unit).wait_recv()
            total[...] = total[...] + left_in[unit].astype(jnp.float32)

        @pl.when(jnp.logical_and(block <= me, me < count - 1))
        def _():
            l_copy(unit).wait_recv()
            total[...] = total[...] + right_in[unit].astype(jnp.float32)

        @pl.when(block > me)
        def _():
            right_out[unit] = total[...].astype(jnp.bfloat16)
            r_copy(unit).start()

        @pl.when(block < me)
        def _():
            left_out[unit] = total[...].astype(jnp.bfloat16)
            l_copy(unit).start()

        @pl.when(block == me)
        def _():
            out_ref[pl.ds(pl.multiple_of(piece * step_rows, step_rows), step_rows), :] = total[...]

    ordered(pass_on)

    def drain(unit, carry):
        block = unit // pieces
        if paired:
            y_copy(unit).wait_send()

        @pl.when(block > me)
        def _():
            r_copy(unit).wait_send()

        @pl.when(block < me)
        def _():
            l_copy(unit).wait_send()

        return carry

    lax.fori_loop(0, count * pieces, drain, 0)


def reduce_all(left, right, count, pieces, paired, collective_id):
    length = left.shape[0] // (2 if paired else 1)
    width = right.shape[1] // count
    units = count * pieces
    blocks = pltpu.VMEM((units, length // pieces, width), jnp.bfloat16)
    sems = pltpu.SemaphoreType.DMA((units,))
    return pl.pallas_call(
        functools.partial(reduce_kernel, count, pieces, paired),
        out_shape=jax.ShapeDtypeStruct((length, width), jnp.float32),
        in_specs=[pl.BlockSpec(memory_space=pltpu.VMEM)] * 2,
        out_specs=pl.BlockSpec(memory_space=pltpu.VMEM),
        scratch_shapes=([blocks, blocks, sems, sems] if paired else [])
        + [pltpu.VMEM((length // pieces, width), jnp.float32)]
        + [blocks] * 4
        + [sems] * 4,
        compiler_params=pltpu.CompilerParams(
            collective_id=collective_id, has_side_effects=True, vmem_limit_bytes=60 * 2**20
        ),
    )(left, right)


def on_device(
    tokens,
    attn_gain,
    query_weight,
    key_weight,
    value_projection_matrix,
    attention_output_matrix,
    bucket_bias_matrix,
    ffn_gain,
    gate_weight,
    up_weight,
    down_projection_weight,
):
    sequences, length, part_width = tokens.shape
    ma_count = lax.axis_size("ma")
    local_heads = bucket_bias_matrix.shape[1]
    inner_width = query_weight.shape[1]
    head_size = inner_width // local_heads
    slab_rows = sequences * length
    token_rows = tokens.reshape(slab_rows, part_width)
    token_float = token_rows.astype(jnp.float32)
    row_count = lax.axis_size("row")
    half = query_weight.shape[0]
    swap = [(i, i ^ 1) for i in range(row_count)]
    my_row = lax.axis_index("row")
    ba_count = lax.axis_size("ba")
    lane = lax.axis_index("ba") % 4
    piece_rows = attention_output_matrix.shape[0] // 4
    out_piece = lax.dynamic_slice_in_dim(attention_output_matrix, lane * piece_rows, piece_rows, 0)
    out_piece = lax.ppermute(out_piece, "row", swap)
    out_across = lax.ppermute(out_piece, "ba", [(i, i ^ 2) for i in range(ba_count)])
    core_swap = [(i, i ^ 1) for i in range(ba_count)]
    out_pieces = [out_piece, lax.ppermute(out_piece, "ba", core_swap), out_across]
    out_pieces.append(lax.ppermute(out_across, "ba", core_swap))
    gains = jnp.concatenate(
        [attn_gain.reshape(1, part_width), ffn_gain.reshape(1, part_width)]
        + [jnp.zeros((14, part_width), jnp.bfloat16)]
    )
    padded = slab_rows + gains.shape[0]
    gathered = gather_all(
        jnp.concatenate([token_rows, gains]), ma_count, (0, slab_rows // 2, padded), True, 3
    )
    whole = lax.dynamic_slice_in_dim(gathered, my_row * padded, padded, 0)
    ffn_gain_full = whole[slab_rows + 1]
    own_float = whole[:slab_rows].astype(jnp.float32)
    scale = lax.rsqrt(jnp.mean(own_float * own_float, axis=-1, keepdims=True) + epsilon)
    gain_half = lax.dynamic_slice_in_dim(whole[slab_rows], my_row * half, half, 0)

    def with_gain(rows):
        return (rows.astype(jnp.float32) * gain_half.astype(jnp.float32)).astype(jnp.bfloat16)

    mine = with_gain(lax.dynamic_slice(whole, (0, my_row * half), (slab_rows, half)))
    arrived = with_gain(
        lax.dynamic_slice(
            gathered, ((1 - my_row) * padded, my_row * half), (slab_rows, half)
        )
    )
    weights_qkv = (query_weight, key_weight, value_projection_matrix)
    outgoing = [
        jnp.dot(arrived, matrix, preferred_element_type=jnp.float32).astype(jnp.bfloat16)
        for matrix in weights_qkv
    ]
    incoming = [lax.ppermute(part, "row", swap) for part in outgoing]
    projected = [
        (jnp.dot(mine, matrix, preferred_element_type=jnp.float32) + part.astype(jnp.float32)) * scale
        for matrix, part in zip(weights_qkv, incoming)
    ]
    query_heads, key_heads, value_heads = [
        member.astype(jnp.bfloat16).reshape(sequences, length, local_heads, head_size)
        for member in projected
    ]
    bucket_grid = buckets(length)
    table_rows = jnp.arange(bucket_bias_matrix.shape[0], dtype=jnp.int32)
    bucket_indicator = (table_rows[:, None, None] == bucket_grid[None, :, :]).astype(jnp.float32)
    relative_position_scores = jnp.einsum(
        "dmy,du->umy", bucket_indicator, bucket_bias_matrix, precision=lax.Precision.HIGHEST
    )
    scores = (
        jnp.einsum("sqhd,skhd->shqk", query_heads, key_heads, preferred_element_type=jnp.float32)
        + relative_position_scores[None]
    )
    row_max = jnp.max(scores, axis=-1, keepdims=True)
    exponent = jnp.exp(scores - row_max)
    weights = (exponent / jnp.sum(exponent, axis=-1, keepdims=True)).astype(jnp.bfloat16)
    attended = jnp.einsum(
        "shqk,skhd->sqhd", weights, value_heads, preferred_element_type=jnp.float32
    )
    attended = attended.astype(jnp.bfloat16).reshape(slab_rows, inner_width)
    out_far = jnp.zeros_like(attention_output_matrix)
    for offset, member in enumerate(out_pieces):
        out_far = lax.dynamic_update_slice_in_dim(
            out_far, member, (lane ^ offset) * piece_rows, 0
        )
    out_full = jnp.where(
        my_row == 0,
        jnp.concatenate([attention_output_matrix, out_far], axis=1),
        jnp.concatenate([out_far, attention_output_matrix], axis=1),
    )
    attn_out = reduce_all(attended, out_full, ma_count, 2, False, 2)
    residual_stream = (token_float + attn_out).astype(jnp.bfloat16)
    residual_f = residual_stream.astype(jnp.float32)
    gate_full, up_full, down_full = (gate_weight, up_weight, down_projection_weight)
    group_rows = gather_all(
        residual_stream, ma_count, (0, slab_rows // 2, slab_rows), False, 0
    )
    ffn_in = rms_scale(group_rows.astype(jnp.float32), ffn_gain_full)
    gate_act = jnp.dot(ffn_in, gate_full, preferred_element_type=jnp.float32)
    up_act = jnp.dot(ffn_in, up_full, preferred_element_type=jnp.float32)
    hidden = (jax.nn.gelu(gate_act, approximate=True) * up_act).astype(jnp.bfloat16)
    ffn_out = reduce_all(hidden, down_full, ma_count, 2, True, 1)
    encoded = (residual_f + ffn_out).astype(jnp.bfloat16)
    return encoded.reshape(sequences, length, part_width)


def solution(mesh):
    in_specs = (
        P(("ba", "row"), None, "ma"),
        P("ma"),
        P("row", "ma"),
        P("row", "ma"),
        P("row", "ma"),
        P("ma", "row"),
        P(None, "ma"),
        P("ma"),
        P(None, ("ma", "row")),
        P(None, ("ma", "row")),
        P(("ma", "row"), None),
    )
    out_specs = P(("ba", "row"), None, "ma")
    return jax.shard_map(
        on_device, mesh=mesh, in_specs=in_specs, out_specs=out_specs, check_vma=False
    )
```
